32 devices in a mesh: dp: 4 (over x, core), rows: 8 (over z, y).
Axes of the slice: x: 2, y: 2, z: 4, core: 2. Of those that a mesh axis runs over, the one named last changes fastest.
Arguments:
- item_table: float32 [131072, 128], P(('dp', 'rows')), may hold values from -3 to 3
- adagrad_state: float32 [131072, 128], P(('dp', 'rows')), may hold values from 0.0001 to 0.01
- history_ids: int32 [4096, 50], P(('dp', 'rows')), may hold values from 0 to 131071, as said below
- positive_ids: int32 [4096], P(('dp', 'rows')), may hold values from 0 to 131071, as said below
Outputs:
- new_table: float32 [131072, 128], P(('dp', 'rows'))
- new_state: float32 [131072, 128], P(('dp', 'rows'))
The draws below stay inside these ranges and needn't reach their ends.
Inputs may be any that keep to these rules, and one draw needn't show every extreme that they name: `history_ids`: ids are counted over one device's 128 users (an aligned block of users), history and positive together, with repeats. In every such block, at most 512 ids have any one value of id // 4096, and some value has exactly 512; one value has exactly 512 in every block. Popular items repeat. `positive_ids`: counted together with history_ids as stated there.
All inputs are finite; a program needn't handle non-finite values.
Results may differ from the reference program's by a relative error of at most 0.00012.
Values sent between devices are 32-bit elements; how exact they have to be, the bound alone decides.
A program may use at most 128 MiB of HBM per device.

```python
import math
import jax
import jax.numpy as jnp
from jax import lax

EMB = 128
HIST = 50
USER_DEV = 128
ROW_DEV = 4096
USERS = 4096
ITEMS = 131072
CAP = 512


def request_ids(key):
    base = jax.random.fold_in(key, 7001)
    keys = jax.random.split(base, 7)
    blocks = USERS // USER_DEV
    slots = blocks * CAP
    per_block = USER_DEV * (HIST + 1)
    slot_owner = jnp.arange(slots, dtype=jnp.int32) // CAP
    noise = jax.random.randint(keys[0], (blocks, slots), 0, 1024, dtype=jnp.int32)
    level = jax.random.randint(keys[1], (blocks, blocks), 0, 4, dtype=jnp.int32) * 512
    hot_common = jax.random.randint(keys[2], (), 0, blocks, dtype=jnp.int32)
    hot_own = jax.random.randint(keys[3], (blocks,), 0, blocks, dtype=jnp.int32)
    hot_flag = jnp.logical_or(slot_owner[None, :] == hot_common, slot_owner[None, :] == hot_own[:, None]).astype(jnp.int32)
    score = (noise + level[:, slot_owner] + 8192 * hot_flag) * slots + jnp.arange(slots, dtype=jnp.int32)[None, :]
    picked_score, chosen = lax.top_k(score, per_block)
    owners = (chosen // CAP).astype(jnp.int32)
    order_keys = jax.random.randint(keys[4], (blocks, per_block), 0, 32768, dtype=jnp.int32) * per_block + jnp.arange(per_block, dtype=jnp.int32)[None, :]
    order = jnp.argsort(order_keys, axis=1, stable=True)
    owners = jnp.take_along_axis(owners, order, axis=1)
    first = jax.random.randint(keys[5], (blocks, per_block), 0, ROW_DEV, dtype=jnp.int32)
    second = jax.random.randint(keys[6], (blocks, per_block), 0, ROW_DEV, dtype=jnp.int32)
    offset = first * second // ROW_DEV
    return (owners * ROW_DEV + offset).astype(jnp.int32).reshape(USERS, HIST + 1)


def draw_history_ids(key, part):
    return request_ids(key)[:, :HIST]


def draw_positive_ids(key, part):
    return request_ids(key)[:, HIST]


def levels(stream_key, dims, cuts, least, high):
    def one(position, parts):
        heights = jax.random.uniform(jax.random.fold_in(jax.random.fold_in(stream_key, 6), position), (parts,), jnp.float32, least / len(cuts), high / len(cuts))
        return jnp.repeat(jnp.exp(heights), dims[position] // parts).reshape((-1,) + (1,) * (len(dims) - position - 1))

    gain = one(*cuts[0])
    for cut in cuts[1:]:
        gain = gain * one(*cut)
    return gain


def normal_values(own_key, dims, width, limit, cuts=(), kind=jnp.bfloat16):
    array = jax.random.normal(own_key, dims, jnp.float32) * width
    if len(cuts) > 0:
        array = levels(own_key, dims, cuts, -0.22, 0.18) * array
    return jnp.clip(array, min=-limit, max=limit).astype(kind)


def setup_inputs(seed: int = 0) -> dict:
    streams_of = jax.random.split(jax.random.key(seed), 5)
    return {
        "item_table": normal_values(streams_of[0], (ITEMS, EMB), 0.5, 3.0, ((0, 32),), jnp.float32),
        "adagrad_state": jnp.clip(jnp.exp(math.log(0.01) - 4.6051702 * jax.random.uniform(streams_of[1], (ITEMS, EMB), jnp.float32) ** levels(streams_of[1], (ITEMS, EMB), ((0, 32),), -0.2, 0.2)), 0.0001, 0.01),
        "history_ids": draw_history_ids(jax.random.fold_in(streams_of[4], 71), 0),
        "positive_ids": draw_positive_ids(jax.random.fold_in(streams_of[4], 71), 0),
    }


penalty_weight = 10.0
step_size = 0.05

def reference(item_table, adagrad_state, history_ids, positive_ids):
    hist_rows = jnp.take(item_table, history_ids, axis=0)
    user_vecs = lax.optimization_barrier(jnp.sum(hist_rows, axis=1)) / HIST
    positive_vecs = jnp.take(item_table, positive_ids, axis=0)
    score_gap = lax.optimization_barrier(jnp.sum(user_vecs * positive_vecs, axis=1)) - 1.0
    user_gram = jnp.dot(user_vecs.T, user_vecs, precision=lax.Precision.HIGHEST, preferred_element_type=jnp.float32)
    item_gram = jnp.dot(item_table.T, item_table, precision=lax.Precision.HIGHEST, preferred_element_type=jnp.float32)
    penalty_coef = penalty_weight / ITEMS
    user_grad = 2.0 * score_gap[:, None] * positive_vecs + 2.0 * penalty_coef * jnp.dot(user_vecs, item_gram, precision=lax.Precision.HIGHEST, preferred_element_type=jnp.float32)
    positive_grad = 2.0 * score_gap[:, None] * user_vecs
    per_history = jnp.broadcast_to((user_grad / HIST)[:, None, :], hist_rows.shape).reshape(-1, EMB)
    row_grad = 2.0 * penalty_coef * jnp.dot(item_table, user_gram, precision=lax.Precision.HIGHEST, preferred_element_type=jnp.float32)
    row_grad = row_grad.at[history_ids.reshape(-1)].add(per_history)
    row_grad = row_grad.at[positive_ids].add(positive_grad)
    new_state = adagrad_state + row_grad * row_grad
    new_table = item_table - step_size * row_grad / jnp.sqrt(new_state)
    return (new_table, new_state)
```

```python
import functools

import jax
import jax.numpy as jnp
from jax import lax
from jax.experimental import pallas as pl
from jax.experimental.pallas import tpu as pltpu
from jax.sharding import PartitionSpec as P

penalty_weight = 10.0
step_size = 0.05
LOW = 128
STREAMS = 8
HIGHEST = lax.Precision.HIGHEST
f32, bf16, i32 = jnp.float32, jnp.bfloat16, jnp.int32


def round_up(value, unit):
    return (value + unit - 1) // unit * unit


def route_kernel(devices, capacity, users_dev, block, owner_ref, local_ref, code_ref, out_ref, acc):
    blocks = owner_ref.shape[1] // block
    upper = (
        lax.broadcasted_iota(i32, (block, block), 0) <= lax.broadcasted_iota(i32, (block, block), 1)
    ).astype(bf16)
    owners = lax.broadcasted_iota(i32, (devices, block), 0)
    ranks_to = lax.broadcasted_iota(i32, (capacity, block), 0)
    acc[...] = jnp.zeros_like(acc)
    carry = jnp.zeros((devices, 1), f32)
    for j in range(blocks):
        cols = slice(j * block, (j + 1) * block)
        local = local_ref[:, cols]
        high = (local // LOW).astype(f32)
        low = (local % LOW).astype(f32)
        code = code_ref[:, cols].astype(f32)
        member = (owner_ref[:, cols] == owners).astype(f32)
        prefix = jnp.dot(member.astype(bf16), upper, preferred_element_type=f32)
        rank = jnp.sum(member * (prefix + carry), axis=0, keepdims=True) - 1.0
        carry = carry + jnp.sum(member, axis=1, keepdims=True)
        left = jnp.concatenate(
            [member * high, member * low, member * code, member], axis=0
        ).astype(bf16)
        right = (rank.astype(i32) == ranks_to).astype(f32).astype(bf16)
        acc[...] += lax.dot_general(
            left, right, (((1,), (1,)), ((), ())), preferred_element_type=f32
        )
    row = acc[0:devices] * LOW + acc[devices : 2 * devices]
    code = acc[2 * devices : 3 * devices]
    present = acc[3 * devices : 4 * devices]
    empty = 2 * users_dev
    out_ref[0] = row.astype(i32)
    out_ref[1] = jnp.where(present > 0.5, code, float(empty)).astype(i32)


def split2(x):
    hi = x.astype(bf16)
    return hi, (x - hi.astype(f32)).astype(bf16)


def partial_kernel(devices, capacity, groups, unroll, rows_ref, code_ref, table_ref, out_ref, picked):
    width = table_ref.shape[1]
    codes_to = lax.broadcasted_iota(i32, (groups, capacity), 0)

    def one(b, _):
        base = b * capacity

        def gather(s, _):
            for k in range(unroll):
                e = s * unroll + k
                r = rows_ref[base + e]
                picked[pl.ds(e, 1), :] = table_ref[pl.ds(r, 1), :]
            return 0

        lax.fori_loop(0, capacity // unroll, gather, 0)
        x = picked[...]
        a0, a1 = split2(x)
        a2 = (x - a0.astype(f32) - a1.astype(f32)).astype(bf16)
        hot = (code_ref[b] == codes_to).astype(f32).astype(bf16)
        both = jnp.dot(hot, jnp.concatenate([a0, a1], axis=1), preferred_element_type=f32)
        last = jnp.dot(hot, a2, preferred_element_type=f32)
        out_ref[pl.ds(pl.multiple_of(b * groups, 8), groups), :] = both[:, :width] + (both[:, width:] + last)
        return 0

    lax.fori_loop(0, devices, one, 0)


def update_kernel(
    devices, users_dev, hist_len, coef, entries, unroll,
    rows_ref, gidx_ref, sums_ref, gram_ref, table_ref, state_ref, new_table_ref, new_state_ref,
    grads, ugram, *accs,
):
    groups = 2 * users_dev
    total = devices * groups
    item_total = gram_ref[...]
    ugram[...] = jnp.zeros_like(ugram)
    grads[pl.ds(total, 8), :] = jnp.zeros((8, grads.shape[1]), f32)

    def user(b, _):
        at = pl.multiple_of(b * groups, 8)
        at2 = pl.multiple_of(b * groups + users_dev, 8)
        uv = sums_ref[pl.ds(at, users_dev), :] / hist_len
        pv = sums_ref[pl.ds(at2, users_dev), :]
        gap = jnp.sum(uv * pv, axis=1, keepdims=True) - 1.0
        ug = 2.0 * gap * pv + 2.0 * coef * jnp.dot(
            uv, item_total, precision=HIGHEST, preferred_element_type=f32
        )
        grads[pl.ds(at, users_dev), :] = ug / hist_len
        grads[pl.ds(at2, users_dev), :] = 2.0 * gap * uv
        ugram[...] += lax.dot_general(
            uv, uv, (((0,), (0,)), ((), ())), precision=HIGHEST, preferred_element_type=f32
        )
        return 0

    lax.fori_loop(0, devices, user, 0)
    for acc in accs:
        acc[...] = jnp.zeros_like(acc)
    part = entries // len(accs)

    def scatter(s, _):
        for q in range(unroll):
            rows = [rows_ref[k * part + s * unroll + q] for k in range(len(accs))]
            gidx = [gidx_ref[k * part + s * unroll + q] for k in range(len(accs))]
            vals = [
                acc[pl.ds(r, 1), :] + grads[pl.ds(g, 1), :] for acc, r, g in zip(accs, rows, gidx)
            ]
            for acc, r, v in zip(accs, rows, vals):
                acc[pl.ds(r, 1), :] = v
        return 0

    lax.fori_loop(0, part // unroll, scatter, 0)
    tile = 256
    rows_dev = table_ref.shape[0]
    user_total = ugram[...]

    def finish(t, _):
        at = pl.ds(pl.multiple_of(t * tile, 8), tile)
        item = table_ref[at, :]
        g = 2.0 * coef * jnp.dot(item, user_total, precision=HIGHEST, preferred_element_type=f32)
        add = accs[0][at, :]
        for acc in accs[1:]:
            add = add + acc[at, :]
        g = g + add
        state = state_ref[at, :] + g * g
        new_state_ref[at, :] = state
        new_table_ref[at, :] = item - step_size * g / jnp.sqrt(state)
        return 0

    lax.fori_loop(0, rows_dev // tile, finish, 0)


VM = pl.BlockSpec(memory_space=pltpu.VMEM)
SM = pl.BlockSpec(memory_space=pltpu.SMEM)
PARAMS = pltpu.CompilerParams(vmem_limit_bytes=60 * 1024 * 1024)


def shards(item_table, adagrad_state, history_ids, positive_ids):
    rows_dev, width = item_table.shape
    users_dev, hist_len = history_ids.shape
    devices = lax.axis_size("dp") * lax.axis_size("rows")
    groups = 2 * users_dev
    count = users_dev * (hist_len + 1)
    capacity = max(8, (count * 5 // (2 * devices) + 7) // 8 * 8)
    block = 512
    padded = round_up(count, block)
    requests = jnp.concatenate([history_ids.reshape(-1), positive_ids])
    code = jnp.concatenate(
        [jnp.arange(users_dev * hist_len, dtype=i32) // hist_len, users_dev + jnp.arange(users_dev, dtype=i32)]
    )
    requests = jnp.pad(requests, (0, padded - count), constant_values=devices * rows_dev)
    code = jnp.pad(code, (0, padded - count))
    owner = requests // rows_dev
    local = requests - owner * rows_dev

    lists = pl.pallas_call(
        functools.partial(route_kernel, devices, capacity, users_dev, block),
        out_shape=jax.ShapeDtypeStruct((2, devices, capacity), i32),
        in_specs=[VM] * 3,
        out_specs=VM,
        scratch_shapes=[pltpu.VMEM((4 * devices, capacity), f32)],
        compiler_params=PARAMS,
        name="route",
    )(owner[None], local[None], code[None])
    asked = lax.all_to_all(lists, ("dp", "rows"), split_axis=1, concat_axis=1, tiled=True)
    rows = asked[0].reshape(-1)
    codes = asked[1]
    entries = devices * capacity
    partial = pl.pallas_call(
        functools.partial(partial_kernel, devices, capacity, groups, 16),
        out_shape=jax.ShapeDtypeStruct((devices * groups, width), f32),
        in_specs=[SM, VM, VM],
        out_specs=VM,
        scratch_shapes=[pltpu.VMEM((capacity, width), f32)],
        compiler_params=PARAMS,
        name="partial",
    )(rows, codes[:, None, :], item_table)
    item_gram = jnp.dot(item_table.T, item_table, precision=HIGHEST, preferred_element_type=f32)
    sums, item_total = lax.psum((partial, item_gram), ("dp", "rows"))
    coef = penalty_weight / (rows_dev * devices)
    gidx = jnp.where(
        codes < groups, codes + groups * jnp.arange(devices, dtype=i32)[:, None], devices * groups
    ).reshape(-1)
    return pl.pallas_call(
        functools.partial(update_kernel, devices, users_dev, hist_len, coef, entries, 2),
        out_shape=(
            jax.ShapeDtypeStruct(item_table.shape, f32),
            jax.ShapeDtypeStruct(item_table.shape, f32),
        ),
        in_specs=[SM, SM, VM, VM, VM, VM],
        out_specs=(VM, VM),
        scratch_shapes=[
            pltpu.VMEM((devices * groups + 8, width), f32),
            pltpu.VMEM((width, width), f32),
        ]
        + [pltpu.VMEM((rows_dev, width), f32)] * STREAMS,
        compiler_params=PARAMS,
        name="update",
    )(rows, gidx, sums, item_total, item_table, adagrad_state)


def solution(mesh):
    return jax.shard_map(
        shards,
        mesh=mesh,
        in_specs=(
            P(("dp", "rows"), None),
            P(("dp", "rows"), None),
            P(("dp", "rows"), None),
            P(("dp", "rows")),
        ),
        out_specs=(P(("dp", "rows"), None), P(("dp", "rows"), None)),
        check_vma=False,
    )
```

```python
import functools

import jax
import jax.numpy as jnp
from jax import lax
from jax.experimental import pallas as pl
from jax.experimental.pallas import tpu as pltpu
from jax.sharding import PartitionSpec as P

penalty_weight = 10.0
step_size = 0.05
LOW = 128
STREAMS = 8
HIGHEST = lax.Precision.HIGHEST
f32, bf16, i32 = jnp.float32, jnp.bfloat16, jnp.int32


def round_up(value, unit):
    return (value + unit - 1) // unit * unit


def route_kernel(devices, capacity, users_dev, block, owner_ref, local_ref, code_ref, out_ref, acc):
    blocks = owner_ref.shape[1] // block
    upper = (
        lax.broadcasted_iota(i32, (block, block), 0) <= lax.broadcasted_iota(i32, (block, block), 1)
    ).astype(bf16)
    owners = lax.broadcasted_iota(i32, (devices, block), 0)
    ranks_to = lax.broadcasted_iota(i32, (capacity, block), 0)
    acc[...] = jnp.zeros_like(acc)
    carry = jnp.zeros((devices, 1), f32)
    for j in range(blocks):
        cols = slice(j * block, (j + 1) * block)
        local = local_ref[:, cols]
        high = (local // LOW).astype(f32)
        low = (local % LOW).astype(f32)
        code = code_ref[:, cols].astype(f32)
        member = (owner_ref[:, cols] == owners).astype(f32)
        prefix = jnp.dot(member.astype(bf16), upper, preferred_element_type=f32)
        rank = jnp.sum(member * (prefix + carry), axis=0, keepdims=True) - 1.0
        carry = carry + jnp.sum(member, axis=1, keepdims=True)
        left = jnp.concatenate(
            [member * high, member * low, member * code, member], axis=0
        ).astype(bf16)
        right = (rank.astype(i32) == ranks_to).astype(f32).astype(bf16)
        acc[...] += lax.dot_general(
            left, right, (((1,), (1,)), ((), ())), preferred_element_type=f32
        )
    row = acc[0:devices] * LOW + acc[devices : 2 * devices]
    code = acc[2 * devices : 3 * devices]
    present = acc[3 * devices : 4 * devices]
    empty = 2 * users_dev
    out_ref[0] = row.astype(i32)
    out_ref[1] = jnp.where(present > 0.5, code, float(empty)).astype(i32)


def split2(x):
    hi = x.astype(bf16)
    return hi, (x - hi.astype(f32)).astype(bf16)


def partial_kernel(devices, capacity, groups, unroll, rows_ref, code_ref, gram_ref, table_ref, out_ref, picked):
    width = table_ref.shape[1]
    codes_to = lax.broadcasted_iota(i32, (groups, capacity), 0)

    def one(b, _):
        base = b * capacity

        def gather(s, _):
            for k in range(unroll):
                e = s * unroll + k
                r = rows_ref[base + e]
                picked[pl.ds(e, 1), :] = table_ref[pl.ds(r, 1), :]
            return 0

        lax.fori_loop(0, capacity // unroll, gather, 0)
        x = picked[...]
        a0, a1 = split2(x)
        a2 = (x - a0.astype(f32) - a1.astype(f32)).astype(bf16)
        hot = (code_ref[b] == codes_to).astype(f32).astype(bf16)
        both = jnp.dot(hot, jnp.concatenate([a0, a1], axis=1), preferred_element_type=f32)
        last = jnp.dot(hot, a2, preferred_element_type=f32)
        out_ref[b, 0:groups, :] = both[:, :width] + (both[:, width:] + last)
        out_ref[b, groups:, :] = gram_ref[b]
        return 0

    lax.fori_loop(0, devices, one, 0)


def reduce_kernel(data, shard, part_ref, out_ref, held, got, send1, recv1, send2, recv2, send3, recv3, send4, recv4):
    peers = data // 2 * shard
    dp, rw = lax.axis_index("dp"), lax.axis_index("rows")
    core = lax.rem(dp, 2)
    flat = dp // 2 * shard + rw
    other = (dp + 1 - 2 * core, rw)
    mesh_id = pl.DeviceIdType.MESH

    def place(k):
        at = lax.rem(flat + k, peers)
        return at // shard * 2 + core, lax.rem(at, shard)

    def slab(k, side):
        d, r = place(k)
        return (d + (1 - 2 * core) * side) * shard + r

    barrier = pltpu.get_barrier_semaphore()
    pl.semaphore_signal(barrier, inc=1, device_id=other, device_id_type=mesh_id)

    def greet(k, _):
        pl.semaphore_signal(barrier, inc=1, device_id=place(k), device_id_type=mesh_id)
        return 0

    lax.fori_loop(1, peers, greet, 0)
    pl.semaphore_wait(barrier, peers)

    def remote(src, dst, send, recv, device):
        return pltpu.make_async_remote_copy(
            src_ref=src, dst_ref=dst, send_sem=send, recv_sem=recv, device_id=device, device_id_type=mesh_id
        )

    def copy1(k):
        return remote(part_ref.at[slab(k, 1)], held.at[k], send1.at[k], recv1.at[k], other)

    def copy2(k):
        return remote(held.at[k], got.at[k], send2.at[k], recv2.at[k], place(k))

    def copy3(k):
        mine = out_ref.at[slab(0, 0)]
        return remote(mine, mine, send3.at[k], recv3.at[k], place(k))

    def copy4(k):
        at = out_ref.at[slab(peers - k, 0)]
        return remote(at, at, send4.at[k], recv4.at[k], other)

    def each(first, count, act):
        def step(k, _):
            act(k)
            return 0

        lax.fori_loop(first, count, step, 0)

    def start1(k):
        copy1(lax.rem(k, peers)).start()

    each(1, peers + 1, start1)

    def pair(k):
        copy1(k).wait_recv()
        held[k] = held[k] + part_ref[slab(k, 0)]
        copy2(k).start()

    each(1, peers, pair)
    copy1(0).wait_recv()
    held[0] = held[0] + part_ref[slab(0, 0)]

    def gain(k):
        copy2(k).wait_recv()
        held[0] = held[0] + got[k]

    each(1, peers, gain)
    out_ref[slab(0, 0)] = held[0]
    each(1, peers, lambda k: copy3(k).start())
    copy4(0).start()

    def forward(k):
        copy3(k).wait_recv()
        copy4(k).start()

    each(1, peers, forward)
    each(0, peers, lambda k: copy4(k).wait_recv())

    def drain(k):
        copy1(k).wait_send()
        copy4(k).wait_send()

    each(0, peers, drain)

    def drain2(k):
        copy2(k).wait_send()
        copy3(k).wait_send()

    each(1, peers, drain2)


def update_kernel(
    devices, users_dev, hist_len, coef, entries, unroll,
    rows_ref, gidx_ref, sums_ref, table_ref, state_ref, new_table_ref, new_state_ref,
    grads, ugram, *accs,
):
    groups = 2 * users_dev
    total = devices * groups
    extra = sums_ref.shape[1] - groups
    for t in range(ugram.shape[0] // extra):
        ugram[t * extra : (t + 1) * extra, :] = sums_ref[t, groups:, :]
    item_total = ugram[...]
    ugram[...] = jnp.zeros_like(ugram)
    grads[pl.ds(total, 8), :] = jnp.zeros((8, grads.shape[1]), f32)

    def user(b, _):
        at = pl.multiple_of(b * groups, 8)
        at2 = pl.multiple_of(b * groups + users_dev, 8)
        uv = sums_ref[b, 0:users_dev, :] / hist_len
        pv = sums_ref[b, users_dev:groups, :]
        gap = jnp.sum(uv * pv, axis=1, keepdims=True) - 1.0
        ug = 2.0 * gap * pv + 2.0 * coef * jnp.dot(
            uv, item_total, precision=HIGHEST, preferred_element_type=f32
        )
        grads[pl.ds(at, users_dev), :] = ug / hist_len
        grads[pl.ds(at2, users_dev), :] = 2.0 * gap * uv
        ugram[...] += lax.dot_general(
            uv, uv, (((0,), (0,)), ((), ())), precision=HIGHEST, preferred_element_type=f32
        )
        return 0

    lax.fori_loop(0, devices, user, 0)
    for acc in accs:
        acc[...] = jnp.zeros_like(acc)
    part = entries // len(accs)

    def scatter(s, _):
        for q in range(unroll):
            rows = [rows_ref[k * part + s * unroll + q] for k in range(len(accs))]
            gidx = [gidx_ref[k * part + s * unroll + q] for k in range(len(accs))]
            vals = [
                acc[pl.ds(r, 1), :] + grads[pl.ds(g, 1), :] for acc, r, g in zip(accs, rows, gidx)
            ]
            for acc, r, v in zip(accs, rows, vals):
                acc[pl.ds(r, 1), :] = v
        return 0

    lax.fori_loop(0, part // unroll, scatter, 0)
    tile = 256
    rows_dev = table_ref.shape[0]
    user_total = ugram[...]

    def finish(t, _):
        at = pl.ds(pl.multiple_of(t * tile, 8), tile)
        item = table_ref[at, :]
        g = 2.0 * coef * jnp.dot(item, user_total, precision=HIGHEST, preferred_element_type=f32)
        add = accs[0][at, :]
        for acc in accs[1:]:
            add = add + acc[at, :]
        g = g + add
        state = state_ref[at, :] + g * g
        new_state_ref[at, :] = state
        new_table_ref[at, :] = item - step_size * g / jnp.sqrt(state)
        return 0

    lax.fori_loop(0, rows_dev // tile, finish, 0)


VM = pl.BlockSpec(memory_space=pltpu.VMEM)
SM = pl.BlockSpec(memory_space=pltpu.SMEM)
PARAMS = pltpu.CompilerParams(vmem_limit_bytes=60 * 1024 * 1024)


def shards(item_table, adagrad_state, history_ids, positive_ids):
    rows_dev, width = item_table.shape
    users_dev, hist_len = history_ids.shape
    devices = lax.axis_size("dp") * lax.axis_size("rows")
    groups = 2 * users_dev
    count = users_dev * (hist_len + 1)
    capacity = max(8, (count * 5 // (2 * devices) + 7) // 8 * 8)
    block = 512
    padded = round_up(count, block)
    requests = jnp.concatenate([history_ids.reshape(-1), positive_ids])
    code = jnp.concatenate(
        [jnp.arange(users_dev * hist_len, dtype=i32) // hist_len, users_dev + jnp.arange(users_dev, dtype=i32)]
    )
    requests = jnp.pad(requests, (0, padded - count), constant_values=devices * rows_dev)
    code = jnp.pad(code, (0, padded - count))
    owner = requests // rows_dev
    local = requests - owner * rows_dev

    lists = pl.pallas_call(
        functools.partial(route_kernel, devices, capacity, users_dev, block),
        out_shape=jax.ShapeDtypeStruct((2, devices, capacity), i32),
        in_specs=[VM] * 3,
        out_specs=VM,
        scratch_shapes=[pltpu.VMEM((4 * devices, capacity), f32)],
        compiler_params=PARAMS,
        name="route",
    )(owner[None], local[None], code[None])
    asked = lax.all_to_all(lists, ("dp", "rows"), split_axis=1, concat_axis=1, tiled=True)
    rows = asked[0].reshape(-1)
    codes = asked[1]
    entries = devices * capacity
    item_gram = jnp.dot(item_table.T, item_table, precision=HIGHEST, preferred_element_type=f32)
    extra = round_up(-(-width // devices), 8)
    chunk = groups + extra
    gram_rows = jnp.pad(item_gram, ((0, devices * extra - width), (0, 0))).reshape(devices, extra, width)
    partial = pl.pallas_call(
        functools.partial(partial_kernel, devices, capacity, groups, 16),
        out_shape=jax.ShapeDtypeStruct((devices, chunk, width), f32),
        in_specs=[SM, VM, VM, VM],
        out_specs=VM,
        scratch_shapes=[pltpu.VMEM((capacity, width), f32)],
        compiler_params=PARAMS,
        name="partial",
    )(rows, codes[:, None, :], gram_rows, item_table)
    data, shard = lax.axis_size("dp"), lax.axis_size("rows")
    peers = devices // 2
    sums = pl.pallas_call(
        functools.partial(reduce_kernel, data, shard),
        out_shape=jax.ShapeDtypeStruct((devices, chunk, width), f32),
        in_specs=[VM],
        out_specs=VM,
        scratch_shapes=[pltpu.VMEM((peers, chunk, width), f32)] * 2 + [pltpu.SemaphoreType.DMA((peers,))] * 8,
        compiler_params=pltpu.CompilerParams(
            vmem_limit_bytes=60 * 1024 * 1024, collective_id=0, has_side_effects=True
        ),
        name="reduce",
    )(partial)
    coef = penalty_weight / (rows_dev * devices)
    gidx = jnp.where(
        codes < groups, codes + groups * jnp.arange(devices, dtype=i32)[:, None], devices * groups
    ).reshape(-1)
    return pl.pallas_call(
        functools.partial(update_kernel, devices, users_dev, hist_len, coef, entries, 2),
        out_shape=(
            jax.ShapeDtypeStruct(item_table.shape, f32),
            jax.ShapeDtypeStruct(item_table.shape, f32),
        ),
        in_specs=[SM, SM, VM, VM, VM],
        out_specs=(VM, VM),
        scratch_shapes=[
            pltpu.VMEM((devices * groups + 8, width), f32),
            pltpu.VMEM((width, width), f32),
        ]
        + [pltpu.VMEM((rows_dev, width), f32)] * STREAMS,
        compiler_params=PARAMS,
        name="update",
    )(rows, gidx, sums, item_table, adagrad_state)


def solution(mesh):
    return jax.shard_map(
        shards,
        mesh=mesh,
        in_specs=(
            P(("dp", "rows"), None),
            P(("dp", "rows"), None),
            P(("dp", "rows"), None),
            P(("dp", "rows")),
        ),
        out_specs=(P(("dp", "rows"), None), P(("dp", "rows"), None)),
        check_vma=False,
    )
```

```python
import functools

import jax
import jax.numpy as jnp
from jax import lax
from jax.experimental import pallas as pl
from jax.experimental.pallas import tpu as pltpu
from jax.sharding import PartitionSpec as P

penalty_weight = 10.0
step_size = 0.05
LOW = 128
STREAMS = 8
HIGHEST = lax.Precision.HIGHEST
f32, bf16, i32 = jnp.float32, jnp.bfloat16, jnp.int32


def round_up(value, unit):
    return (value + unit - 1) // unit * unit


def route_kernel(devices, capacity, users_dev, block, owner_ref, local_ref, code_ref, out_ref, acc):
    blocks = owner_ref.shape[1] // block
    upper = (
        lax.broadcasted_iota(i32, (block, block), 0) <= lax.broadcasted_iota(i32, (block, block), 1)
    ).astype(bf16)
    owners = lax.broadcasted_iota(i32, (devices, block), 0)
    ranks_to = lax.broadcasted_iota(i32, (capacity, block), 0)
    acc[...] = jnp.zeros_like(acc)
    carry = jnp.zeros((devices, 1), f32)
    for j in range(blocks):
        cols = slice(j * block, (j + 1) * block)
        local = local_ref[:, cols]
        high = (local // LOW).astype(f32)
        low = (local % LOW).astype(f32)
        code = code_ref[:, cols].astype(f32)
        member = (owner_ref[:, cols] == owners).astype(f32)
        prefix = jnp.dot(member.astype(bf16), upper, preferred_element_type=f32)
        rank = jnp.sum(member * (prefix + carry), axis=0, keepdims=True) - 1.0
        carry = carry + jnp.sum(member, axis=1, keepdims=True)
        left = jnp.concatenate(
            [member * high, member * low, member * code, member], axis=0
        ).astype(bf16)
        right = (rank.astype(i32) == ranks_to).astype(f32).astype(bf16)
        acc[...] += lax.dot_general(
            left, right, (((1,), (1,)), ((), ())), preferred_element_type=f32
        )
    row = acc[0:devices] * LOW + acc[devices : 2 * devices]
    code = acc[2 * devices : 3 * devices]
    present = acc[3 * devices : 4 * devices]
    empty = 2 * users_dev
    out_ref[0] = row.astype(i32)
    out_ref[1] = jnp.where(present > 0.5, code, float(empty)).astype(i32)


def split2(x):
    hi = x.astype(bf16)
    return hi, (x - hi.astype(f32)).astype(bf16)


def partial_kernel(devices, capacity, groups, unroll, rows_ref, code_ref, gram_ref, table_ref, out_ref, picked):
    width = table_ref.shape[1]
    codes_to = lax.broadcasted_iota(i32, (groups, capacity), 0)

    def one(b, _):
        base = b * capacity

        def gather(s, _):
            for k in range(unroll):
                e = s * unroll + k
                r = rows_ref[base + e]
                picked[pl.ds(e, 1), :] = table_ref[pl.ds(r, 1), :]
            return 0

        lax.fori_loop(0, capacity // unroll, gather, 0)
        x = picked[...]
        a0, a1 = split2(x)
        a2 = (x - a0.astype(f32) - a1.astype(f32)).astype(bf16)
        hot = (code_ref[b] == codes_to).astype(f32).astype(bf16)
        both = jnp.dot(hot, jnp.concatenate([a0, a1], axis=1), preferred_element_type=f32)
        last = jnp.dot(hot, a2, preferred_element_type=f32)
        out_ref[b, 0:groups, :] = both[:, :width] + (both[:, width:] + last)
        out_ref[b, groups:, :] = gram_ref[b]
        return 0

    lax.fori_loop(0, devices, one, 0)


def reduce_kernel(data, shard, part_ref, out_ref, held, got, send1, recv1, send2, recv2, send3, recv3, send4, recv4):
    peers = data // 2 * shard
    dp, rw = lax.axis_index("dp"), lax.axis_index("rows")
    core = lax.rem(dp, 2)
    flat = dp // 2 * shard + rw
    other = (dp + 1 - 2 * core, rw)
    mesh_id = pl.DeviceIdType.MESH

    def place(k):
        at = lax.rem(flat + k, peers)
        return at // shard * 2 + core, lax.rem(at, shard)

    def slab(k, side):
        d, r = place(k)
        return (d + (1 - 2 * core) * side) * shard + r

    barrier = pltpu.get_barrier_semaphore()
    pl.semaphore_signal(barrier, inc=1, device_id=other, device_id_type=mesh_id)

    def greet(k, _):
        pl.semaphore_signal(barrier, inc=1, device_id=place(k), device_id_type=mesh_id)
        return 0

    lax.fori_loop(1, peers, greet, 0)
    pl.semaphore_wait(barrier, peers)

    def remote(src, dst, send, recv, device):
        return pltpu.make_async_remote_copy(
            src_ref=src, dst_ref=dst, send_sem=send, recv_sem=recv, device_id=device, device_id_type=mesh_id
        )

    def copy1(k):
        return remote(part_ref.at[slab(k, 1)], held.at[k], send1.at[k], recv1.at[k], other)

    def copy2(k):
        return remote(held.at[k], got.at[k], send2.at[k], recv2.at[k], place(k))

    def copy3(k):
        mine = out_ref.at[slab(0, 0)]
        return remote(mine, mine, send3.at[k], recv3.at[k], place(k))

    def copy4(k):
        at = out_ref.at[slab(peers - k, 0)]
        return remote(at, at, send4.at[k], recv4.at[k], other)

    def each(first, count, act):
        def step(k, _):
            act(k)
            return 0

        lax.fori_loop(first, count, step, 0)

    def start1(k):
        copy1(lax.rem(k, peers)).start()

    each(1, peers + 1, start1)

    def pair(k):
        copy1(k).wait_recv()
        held[k] = held[k] + part_ref[slab(k, 0)]
        copy2(k).start()

    each(1, peers, pair)
    copy1(0).wait_recv()
    held[0] = held[0] + part_ref[slab(0, 0)]

    def gain(k):
        copy2(k).wait_recv()
        held[0] = held[0] + got[k]

    each(1, peers, gain)
    out_ref[slab(0, 0)] = held[0]
    each(1, peers, lambda k: copy3(k).start())
    copy4(0).start()

    def forward(k):
        copy3(k).wait_recv()
        copy4(k).start()

    each(1, peers, forward)
    each(0, peers, lambda k: copy4(k).wait_recv())

    def drain(k):
        copy1(k).wait_send()
        copy4(k).wait_send()

    each(0, peers, drain)

    def drain2(k):
        copy2(k).wait_send()
        copy3(k).wait_send()

    each(1, peers, drain2)


def update_kernel(
    devices, users_dev, hist_len, coef, entries, unroll,
    rows_ref, gidx_ref, sums_ref, table_ref, state_ref, new_table_ref, new_state_ref,
    grads, ugram, *accs,
):
    groups = 2 * users_dev
    total = devices * groups
    extra = sums_ref.shape[1] - groups
    for t in range(ugram.shape[0] // extra):
        ugram[t * extra : (t + 1) * extra, :] = sums_ref[t, groups:, :]
    item_total = ugram[...]
    ugram[...] = jnp.zeros_like(ugram)
    grads[pl.ds(total, 8), :] = jnp.zeros((8, grads.shape[1]), f32)

    def user(b, _):
        at = pl.multiple_of(b * groups, 8)
        at2 = pl.multiple_of(b * groups + users_dev, 8)
        uv = sums_ref[b, 0:users_dev, :] / hist_len
        pv = sums_ref[b, users_dev:groups, :]
        gap = jnp.sum(uv * pv, axis=1, keepdims=True) - 1.0
        ug = 2.0 * gap * pv + 2.0 * coef * jnp.dot(
            uv, item_total, precision=HIGHEST, preferred_element_type=f32
        )
        grads[pl.ds(at, users_dev), :] = ug / hist_len
        grads[pl.ds(at2, users_dev), :] = 2.0 * gap * uv
        ugram[...] += lax.dot_general(
            uv, uv, (((0,), (0,)), ((), ())), precision=HIGHEST, preferred_element_type=f32
        )
        return 0

    lax.fori_loop(0, devices, user, 0)
    for acc in accs:
        acc[...] = jnp.zeros_like(acc)
    part = entries // len(accs)

    def scatter(s, _):
        for q in range(unroll):
            rows = [rows_ref[k * part + s * unroll + q] for k in range(len(accs))]
            gidx = [gidx_ref[k * part + s * unroll + q] for k in range(len(accs))]
            vals = [
                acc[pl.ds(r, 1), :] + grads[pl.ds(g, 1), :] for acc, r, g in zip(accs, rows, gidx)
            ]
            for acc, r, v in zip(accs, rows, vals):
                acc[pl.ds(r, 1), :] = v
        return 0

    lax.fori_loop(0, part // unroll, scatter, 0)
    tile = 256
    rows_dev = table_ref.shape[0]
    user_total = ugram[...]

    def finish(t, _):
        at = pl.ds(pl.multiple_of(t * tile, 8), tile)
        item = table_ref[at, :]
        g = 2.0 * coef * jnp.dot(item, user_total, precision=HIGHEST, preferred_element_type=f32)
        add = accs[0][at, :]
        for acc in accs[1:]:
            add = add + acc[at, :]
        g = g + add
        state = state_ref[at, :] + g * g
        new_state_ref[at, :] = state
        new_table_ref[at, :] = item - step_size * g / jnp.sqrt(state)
        return 0

    lax.fori_loop(0, rows_dev // tile, finish, 0)


VM = pl.BlockSpec(memory_space=pltpu.VMEM)
SM = pl.BlockSpec(memory_space=pltpu.SMEM)
PARAMS = pltpu.CompilerParams(vmem_limit_bytes=60 * 1024 * 1024)


def shards(item_table, adagrad_state, history_ids, positive_ids):
    rows_dev, width = item_table.shape
    users_dev, hist_len = history_ids.shape
    devices = lax.axis_size("dp") * lax.axis_size("rows")
    groups = 2 * users_dev
    count = users_dev * (hist_len + 1)
    capacity = max(8, (count * 5 // (2 * devices) + 7) // 8 * 8)
    block = 512
    padded = round_up(count, block)
    requests = jnp.concatenate([history_ids.reshape(-1), positive_ids])
    code = jnp.concatenate(
        [jnp.arange(users_dev * hist_len, dtype=i32) // hist_len, users_dev + jnp.arange(users_dev, dtype=i32)]
    )
    requests = jnp.pad(requests, (0, padded - count), constant_values=devices * rows_dev)
    code = jnp.pad(code, (0, padded - count))
    owner = requests // rows_dev
    local = requests - owner * rows_dev

    lists = pl.pallas_call(
        functools.partial(route_kernel, devices, capacity, users_dev, block),
        out_shape=jax.ShapeDtypeStruct((2, devices, capacity), i32),
        in_specs=[VM] * 3,
        out_specs=VM,
        scratch_shapes=[pltpu.VMEM((4 * devices, capacity), f32)],
        compiler_params=PARAMS,
        name="route",
    )(owner[None], local[None], code[None])
    asked = lax.all_to_all(lists, ("dp", "rows"), split_axis=1, concat_axis=1, tiled=True)
    rows = asked[0].reshape(-1)
    codes = asked[1]
    entries = devices * capacity
    item_gram = jnp.dot(item_table.T, item_table, precision=HIGHEST, preferred_element_type=f32)
    extra = round_up(-(-width // devices), 8)
    chunk = groups + extra
    gram_rows = jnp.pad(item_gram, ((0, devices * extra - width), (0, 0))).reshape(devices, extra, width)
    partial = pl.pallas_call(
        functools.partial(partial_kernel, devices, capacity, groups, 32),
        out_shape=jax.ShapeDtypeStruct((devices, chunk, width), f32),
        in_specs=[SM, VM, VM, VM],
        out_specs=VM,
        scratch_shapes=[pltpu.VMEM((capacity, width), f32)],
        compiler_params=PARAMS,
        name="partial",
    )(rows, codes[:, None, :], gram_rows, item_table)
    data, shard = lax.axis_size("dp"), lax.axis_size("rows")
    peers = devices // 2
    sums = pl.pallas_call(
        functools.partial(reduce_kernel, data, shard),
        out_shape=jax.ShapeDtypeStruct((devices, chunk, width), f32),
        in_specs=[VM],
        out_specs=VM,
        scratch_shapes=[pltpu.VMEM((peers, chunk, width), f32)] * 2 + [pltpu.SemaphoreType.DMA((peers,))] * 8,
        compiler_params=pltpu.CompilerParams(
            vmem_limit_bytes=60 * 1024 * 1024, collective_id=0, has_side_effects=True
        ),
        name="reduce",
    )(partial)
    coef = penalty_weight / (rows_dev * devices)
    gidx = jnp.where(
        codes < groups, codes + groups * jnp.arange(devices, dtype=i32)[:, None], devices * groups
    ).reshape(-1)
    return pl.pallas_call(
        functools.partial(update_kernel, devices, users_dev, hist_len, coef, entries, 4),
        out_shape=(
            jax.ShapeDtypeStruct(item_table.shape, f32),
            jax.ShapeDtypeStruct(item_table.shape, f32),
        ),
        in_specs=[SM, SM, VM, VM, VM],
        out_specs=(VM, VM),
        scratch_shapes=[
            pltpu.VMEM((devices * groups + 8, width), f32),
            pltpu.VMEM((width, width), f32),
        ]
        + [pltpu.VMEM((rows_dev, width), f32)] * STREAMS,
        compiler_params=PARAMS,
        name="update",
    )(rows, gidx, sums, item_table, adagrad_state)


def solution(mesh):
    return jax.shard_map(
        shards,
        mesh=mesh,
        in_specs=(
            P(("dp", "rows"), None),
            P(("dp", "rows"), None),
            P(("dp", "rows"), None),
            P(("dp", "rows")),
        ),
        out_specs=(P(("dp", "rows"), None), P(("dp", "rows"), None)),
        check_vma=False,
    )
```
